256 devices in a mesh: dom: 32 (over x, y, core), feat: 8 (over z).
Axes of the slice: x: 4, y: 4, z: 8, core: 2. Of those that a mesh axis runs over, the one named last changes fastest.
Arguments:
- features: bfloat16 [512, 262144], P('feat', 'dom'), may hold values from -3 to 3
- send_blocks: int32 [32, 32, 8], P('dom'), may hold values from 0 to 63, as said below
- counts: int32 [32, 32], P('dom'), may hold values from 0 to 8, as said below
- tile_blocks: int32 [24, 2048], P(None, 'dom'), may hold values from 0 to 319, as said below
- neighbours: int32 [24, 262144], P(None, 'dom'), may hold values from 0 to 127
- degree: int32 [262144], P('dom'), may hold values from 1 to 24
- epsilon: float32 [1], replicated, may hold values from -0.3 to 0.6
- w_first: bfloat16 [512, 512], replicated, may hold values from -0.25 to 0.25
- b_first: float32 [512], replicated, may hold values from -3 to 3
- w_second: bfloat16 [512, 512], replicated, may hold values from -0.25 to 0.25
- b_second: float32 [512], replicated, may hold values from -3 to 3
Outputs:
- updated: bfloat16 [262144, 512], P(('dom', 'feat'))
The draws below stay inside these ranges and needn't reach their ends.
Inputs may be any that keep to these rules, and one draw needn't show every extreme that they name: `send_blocks`: entry [q, p, s] is a row block of partition q; the entries of one pair (q, p) are distinct. counts[q, p] leading slots of send_blocks[q, p] are used; zero where q == p; in every draw some partition receives 8 blocks from every other partition. `tile_blocks`: an entry for a row block of partition p is below 64 (a row block of p) or equals 64 + q * 8 + s for a slot s of a partition q other than p.
All inputs are finite; a program needn't handle non-finite values.
Results may differ from the reference program's by a relative error of at most 0.0055.
Values may be sent and summed in bfloat16 or wider, within the bound.
A program may use at most 64 MiB of HBM per device.

```python
import jax
import jax.numpy as jnp
from jax import lax

D = 512
H = 512
ROWS = 8192
BLOCK = 128
SLOTS = 8
NEIGH = 24
PARTITIONS = 32
NODES = 262144
BLOCKS = 64


def draw_send_blocks(key, part):
    key_list = jax.random.split(jax.random.fold_in(key, 11), PARTITIONS * PARTITIONS)

    def pick(single):
        return jax.random.permutation(single, BLOCKS)[:SLOTS]
    picked = jax.vmap(pick)(key_list)
    return picked.reshape(PARTITIONS, PARTITIONS, SLOTS).astype(jnp.int32)


def draw_counts(key, part):
    first, second = jax.random.split(jax.random.fold_in(key, 23))
    base = jax.random.randint(first, (PARTITIONS, PARTITIONS), 1, SLOTS + 1)
    heavy = jax.random.randint(second, (), 0, PARTITIONS)
    column = jnp.arange(PARTITIONS, dtype=jnp.int32)[None, :]
    rowpos = jnp.arange(PARTITIONS, dtype=jnp.int32)[:, None]
    base = jnp.where(column == heavy, SLOTS, base)
    base = jnp.where(column == rowpos, 0, base)
    return base.astype(jnp.int32)


def draw_tile_blocks(key, part):
    keys = jax.random.split(jax.random.fold_in(key, 37), 4)
    block_count = NODES // BLOCK
    shape = (block_count, NEIGH)
    dst_part = (jnp.arange(block_count, dtype=jnp.int32) // BLOCKS)[:, None]
    which = jax.random.randint(keys[0], shape, 0, 2)
    local = jax.random.randint(keys[1], shape, 0, BLOCKS)
    source = (dst_part + jax.random.randint(keys[2], shape, 1, PARTITIONS)) % PARTITIONS
    slot_pick = jax.random.randint(keys[3], shape, 0, SLOTS)
    remote = BLOCKS + source * SLOTS + slot_pick
    return jnp.where(which == 0, local, remote).astype(jnp.int32).T


def set_ends(entries, key, least, high):
    spot = [jax.random.randint(jax.random.fold_in(key, axis), (), 0, length) for axis, length in enumerate(entries.shape)]
    longest = entries.shape.index(max(entries.shape))
    beside = spot[:longest] + [(spot[longest] + 1) % entries.shape[longest]] + spot[longest + 1:]
    return entries.at[tuple(spot)].set(least).at[tuple(beside)].set(high)


def block_levels(rng, dims, pieces, low, largest):
    gain = 1.0
    for dim, shards_of in pieces:
        draws = jax.random.uniform(jax.random.fold_in(jax.random.fold_in(rng, 6), dim), (shards_of,), jnp.float32, low / len(pieces), largest / len(pieces))
        gain = gain * jnp.repeat(jnp.exp(draws), dims[dim] // shards_of).reshape((-1,) + (1,) * (len(dims) - 1 - dim))
    return gain


def noise(own_key, extent, spread, bound, cuts=(), kind=jnp.bfloat16):
    result = jax.random.normal(own_key, extent, jnp.float32) * spread
    if len(cuts) > 0:
        result = block_levels(own_key, extent, cuts, -0.22, 0.18) * result
    return jnp.clip(result, min=-bound, max=bound).astype(kind)


def setup_inputs(seed: int = 0) -> dict:
    streams_of = jax.random.split(jax.random.key(seed), 12)
    features = noise(streams_of[0], (D, NODES), 0.5, 3.0, ((0, 8), (1, 32)))
    send_blocks = draw_send_blocks(jax.random.fold_in(streams_of[11], 71), 0)
    counts = draw_counts(jax.random.fold_in(streams_of[11], 71), 0)
    tile_blocks = draw_tile_blocks(jax.random.fold_in(streams_of[11], 71), 0)
    neighbours = set_ends(jax.random.randint(streams_of[4], (NEIGH, NODES), 0, BLOCK), jax.random.fold_in(streams_of[4], 1), 0, BLOCK - 1).astype(jnp.int32)
    degree = set_ends(jax.random.randint(streams_of[5], (NODES,), 1, NEIGH + 1), jax.random.fold_in(streams_of[5], 1), 1, NEIGH).astype(jnp.int32)
    epsilon = jnp.clip(jax.random.uniform(streams_of[6], (1,), jnp.float32, -0.3, 0.6), -0.3, 0.6)
    w_first = noise(streams_of[7], (D, H), D ** -0.5, 0.25)
    b_first = noise(streams_of[8], (H,), 0.5, 3.0, (), jnp.float32)
    w_second = noise(streams_of[9], (H, D), H ** -0.5, 0.25)
    b_second = noise(streams_of[10], (D,), 0.5, 3.0, (), jnp.float32)
    return {"features": features, "send_blocks": send_blocks, "counts": counts, "tile_blocks": tile_blocks, "neighbours": neighbours, "degree": degree, "epsilon": epsilon, "w_first": w_first, "b_first": b_first, "w_second": w_second, "b_second": b_second}


def reference(features, send_blocks, counts, tile_blocks, neighbours, degree, epsilon, w_first, b_first, w_second, b_second):
    node_rows = features.T
    tile_rows = jnp.repeat(tile_blocks.T, BLOCK, axis=0)
    lists = (tile_rows * BLOCK + neighbours.T).astype(jnp.int32)
    row_ids = jnp.arange(NODES, dtype=jnp.int32)
    row_part = (row_ids // ROWS)[:, None]
    offset = jnp.maximum(lists - ROWS, 0)
    source = offset // (SLOTS * BLOCK)
    slot_index = (offset // BLOCK) % SLOTS
    in_block = offset % BLOCK
    block_index = send_blocks[source, row_part, slot_index]
    remote = source * ROWS + block_index * BLOCK + in_block
    is_local = lists < ROWS
    target = jnp.where(is_local, row_part * ROWS + lists, remote).astype(jnp.int32)
    live_mask = (jnp.arange(NEIGH, dtype=jnp.int32)[None, :] < degree[:, None]) & (is_local | (slot_index < counts[source, row_part]))
    weight = live_mask.astype(jnp.float32)
    block_rows = min(NODES, 4096)

    def block_sum(pair):
        gathered = node_rows[pair[0]].astype(jnp.float32)
        return jnp.einsum('rk,rkd->rd', pair[1], gathered)

    near_sum = lax.map(block_sum, (target.reshape(-1, block_rows, NEIGH), weight.reshape(-1, block_rows, NEIGH)))
    near_sum = near_sum.reshape(NODES, D)
    combined = ((1.0 + epsilon[0]) * node_rows.astype(jnp.float32) + near_sum).astype(jnp.bfloat16)
    pre_act = jnp.dot(combined, w_first, preferred_element_type=jnp.float32) + b_first
    activated = jax.nn.relu(pre_act).astype(jnp.bfloat16)
    return (jnp.dot(activated, w_second, preferred_element_type=jnp.float32) + b_second).astype(jnp.bfloat16)
```

```python
import functools

import jax
import jax.numpy as jnp
from jax import lax
from jax.experimental import pallas as pl
from jax.experimental.pallas import tpu as pltpu
from jax.sharding import PartitionSpec as P

MESH = pl.DeviceIdType.MESH
BLOCK = 128
DOM = 32
FEAT = 8
SLOTS = 8
NEIGH = 24
BLOCKS = 64
CHUNKS = 4
WIDTH = 16
UNROLL = 4
OWNED = 1024

OFFSETS = [(a, b, c) for a in range(4) for b in range(4) for c in range(2)][1:]
CLASSES = [[o for o in OFFSETS if o[1] == k] for k in (1, 3, 2, 0)]
ORDER = []
while any(CLASSES):
    for group in CLASSES:
        if group:
            ORDER.append(group.pop(0))


def partner(me, offset):
    x = lax.rem(me // 8 + offset[0], 4)
    y = lax.rem((me // 2) % 4 + offset[1], 4)
    core = lax.rem(me % 2 + offset[2], 2)
    return x * 8 + y * 2 + core


def lane_gather(tile, index):
    return lax.gather(
        tile,
        index[..., None],
        lax.GatherDimensionNumbers(
            offset_dims=(),
            collapsed_slice_dims=(1,),
            start_index_map=(1,),
            operand_batching_dims=(0,),
            start_indices_batching_dims=(0,),
        ),
        slice_sizes=(1, 1),
        mode=lax.GatherScatterMode.PROMISE_IN_BOUNDS,
    )


def kernel(
    send_ref, count_ref, tile_ref, eps_ref, feat_ref, near_ref, degree_ref, w1_ref, b1_ref, w2_ref, b2_ref,
    out_ref, *scratch,
):
    tables, sends, mixes, parcels, owns = (scratch[CHUNKS * k : CHUNKS * (k + 1)] for k in range(5))
    index_ref, pre_ref, dom_send, dom_recv, feat_send, feat_recv = scratch[CHUNKS * 5 :]
    me = lax.axis_index("dom")
    lane = lax.axis_index("feat")

    barrier = pltpu.get_barrier_semaphore()
    for offset in ORDER:
        pl.semaphore_signal(barrier, inc=1, device_id={"dom": partner(me, offset)}, device_id_type=MESH)
    for step in range(1, FEAT):
        pl.semaphore_signal(barrier, inc=1, device_id={"feat": lax.rem(lane + step, FEAT)}, device_id_type=MESH)

    def pack(c):
        def own(b, carry):
            lanes = pl.ds(pl.multiple_of(b * BLOCK, BLOCK), BLOCK)
            block = feat_ref[c * WIDTH : (c + 1) * WIDTH, lanes]
            owns[c][b] = block
            tables[c][b] = block
            return carry

        lax.fori_loop(0, BLOCKS, own, 0, unroll=4)

        def body(p, carry):
            used = jnp.full((WIDTH, BLOCK), count_ref[0, p], jnp.int32)
            for s in range(SLOTS):
                block = owns[c][send_ref[s, p]]
                sends[c][p, s] = jnp.where(s < used, block, jnp.zeros_like(block))
            return carry

        lax.fori_loop(0, DOM, body, 0)

    def launch(c):
        for offset in ORDER:
            p = partner(me, offset)
            pltpu.make_async_remote_copy(
                src_ref=sends[c].at[p],
                dst_ref=tables[c].at[pl.ds(BLOCKS + me * SLOTS, SLOTS)],
                send_sem=dom_send.at[c],
                recv_sem=dom_recv.at[c],
                device_id={"dom": p},
                device_id_type=MESH,
            ).start()

    for c in range(CHUNKS):
        pack(c)
        if c == 0:
            pl.semaphore_wait(barrier, DOM + FEAT - 2)
        launch(c)

    def stage(b, carry):
        lanes = pl.ds(pl.multiple_of(b * BLOCK, BLOCK), BLOCK)
        for j in range(NEIGH):
            index_ref[b, j] = jnp.broadcast_to(near_ref[j : j + 1, lanes], (WIDTH, BLOCK)).astype(jnp.int16)
        return carry

    lax.fori_loop(0, BLOCKS, stage, 0)
    for c in range(CHUNKS):
        for s in range(SLOTS):
            tables[c][BLOCKS + me * SLOTS + s] = jnp.zeros((WIDTH, BLOCK), jnp.bfloat16)

    weight = 1.0 + eps_ref[0]

    def to_feat(c, g):
        return pltpu.make_async_remote_copy(
            src_ref=mixes[c].at[g],
            dst_ref=parcels[c].at[lane],
            send_sem=feat_send.at[c],
            recv_sem=feat_recv.at[c],
            device_id={"feat": g},
            device_id_type=MESH,
        )

    def aggregate(c):
        table = tables[c]

        def group(i, carry):
            g = lax.rem(lane + 1 + i, FEAT)

            def part(h, inner):
                for u in range(UNROLL):
                    at = h * UNROLL + u
                    b = g * 8 + at
                    limit = jnp.broadcast_to(
                        degree_ref[:, pl.ds(pl.multiple_of(b * BLOCK, BLOCK), BLOCK)], (8, BLOCK)
                    )
                    own = owns[c][b].astype(jnp.float32)
                    low, high = weight * own[:8], weight * own[8:]
                    for j in range(NEIGH):
                        got = lane_gather(table[tile_ref[j, b]], index_ref[b, j]).astype(jnp.float32)
                        live = j < limit
                        low = low + jnp.where(live, got[:8], 0.0)
                        high = high + jnp.where(live, got[8:], 0.0)
                    mixes[c][g, :, pl.ds(pl.multiple_of(at * BLOCK, BLOCK), BLOCK)] = jnp.concatenate(
                        [low, high], 0
                    ).astype(jnp.bfloat16)
                return inner

            lax.fori_loop(0, 8 // UNROLL, part, 0)

            @pl.when(i < FEAT - 1)
            def _():
                to_feat(c, g).start()

            return carry

        lax.fori_loop(0, FEAT, group, 0)
        parcels[c][lane] = mixes[c][lane]

    def mlp(c):
        held = parcels[c].at[pl.ds(0, FEAT - 1)]
        pltpu.make_async_copy(held, held, feat_recv.at[c]).wait()
        w1 = jnp.concatenate([w1_ref[f * 64 + c * WIDTH : f * 64 + (c + 1) * WIDTH] for f in range(FEAT)], 0)

        def body(r, carry):
            rows = pl.ds(pl.multiple_of(r * 256, 256), 256)
            cols = parcels[c][:, :, rows].reshape(FEAT * WIDTH, 256)
            part = lax.dot_general(cols, w1, (((0,), (0,)), ((), ())), preferred_element_type=jnp.float32)
            if c == 0:
                pre_ref[rows] = part + b1_ref[...]
            elif c < CHUNKS - 1:
                pre_ref[rows] += part
            else:
                act = jnp.maximum(pre_ref[rows] + part, 0.0).astype(jnp.bfloat16)
                out_ref[rows] = (
                    jnp.dot(act, w2_ref[...], preferred_element_type=jnp.float32) + b2_ref[...]
                ).astype(jnp.bfloat16)
            return carry

        lax.fori_loop(0, OWNED // 256, body, 0)

    for c in range(CHUNKS):
        landed = tables[c].at[pl.ds(BLOCKS, (DOM - 1) * SLOTS)]
        pltpu.make_async_copy(landed, landed, dom_recv.at[c]).wait()
        aggregate(c)
        if c > 0:
            mlp(c - 1)
    mlp(CHUNKS - 1)
    for c in range(CHUNKS):
        sent = sends[c].at[pl.ds(0, DOM - 1)]
        pltpu.make_async_copy(sent, sent, dom_send.at[c]).wait()
        left = mixes[c].at[pl.ds(0, FEAT - 1)]
        pltpu.make_async_copy(left, left, feat_send.at[c]).wait()


def per_device(
    features, send_blocks, counts, tile_blocks, neighbours, degree, epsilon, w_first, b_first, w_second, b_second
):
    smem = pl.BlockSpec(memory_space=pltpu.SMEM)
    vmem = pl.BlockSpec(memory_space=pltpu.VMEM)
    bf16 = jnp.bfloat16
    return pl.pallas_call(
        kernel,
        out_shape=jax.ShapeDtypeStruct((OWNED, w_second.shape[1]), bf16),
        in_specs=[smem] * 4 + [vmem] * 7,
        out_specs=vmem,
        scratch_shapes=[pltpu.VMEM((BLOCKS + DOM * SLOTS, WIDTH, BLOCK), bf16)] * CHUNKS
        + [pltpu.VMEM((DOM, SLOTS, WIDTH, BLOCK), bf16)] * CHUNKS
        + [pltpu.VMEM((FEAT, WIDTH, OWNED), bf16)] * CHUNKS
        + [pltpu.VMEM((FEAT, WIDTH, OWNED), bf16)] * CHUNKS
        + [pltpu.VMEM((BLOCKS, WIDTH, BLOCK), bf16)] * CHUNKS
        + [
            pltpu.VMEM((BLOCKS, NEIGH, WIDTH, BLOCK), jnp.int16),
            pltpu.VMEM((OWNED, w_first.shape[1]), jnp.float32),
        ]
        + [pltpu.SemaphoreType.DMA((CHUNKS,))] * 4,
        compiler_params=pltpu.CompilerParams(
            collective_id=0, has_side_effects=True, vmem_limit_bytes=52 * 1024 * 1024
        ),
        name="gin",
    )(
        send_blocks[0].T,
        counts,
        tile_blocks,
        epsilon,
        features,
        neighbours,
        degree[None],
        w_first,
        b_first[None],
        w_second,
        b_second[None],
    )


def solution(mesh):
    return jax.shard_map(
        per_device,
        mesh=mesh,
        in_specs=(
            P("feat", "dom"),
            P("dom", None, None),
            P("dom", None),
            P(None, "dom"),
            P(None, "dom"),
            P("dom"),
            P(),
            P(),
            P(),
            P(),
            P(),
        ),
        out_specs=P(("dom", "feat"), None),
        check_vma=False,
    )
```

```python
import functools

import jax
import jax.numpy as jnp
from jax import lax
from jax.experimental import pallas as pl
from jax.experimental.pallas import tpu as pltpu
from jax.sharding import PartitionSpec as P

MESH = pl.DeviceIdType.MESH
BLOCK = 128
DOM = 32
FEAT = 8
SLOTS = 8
NEIGH = 24
BLOCKS = 64
CHUNKS = 4
WIDTH = 16
UNROLL = 8
OWNED = 1024

RING = 4
PLAN = ("s0", "s1", "t0", "f0", "n0", "d0", "f1", "n1", "r0", "d1", "r1", "d2", "d3", "a0", "d4", "d5", "d6", "d7", "a1", "m0", "a2", "m1", "a3", "m2", "m3")
RINGS = 2
HALF = BLOCKS // 2
WAVE = [(1, 0), (3, 0), (2, 0), (1, 1), (3, 1), (2, 1), (0, 1)]


OFFSETS = [(a, b, c) for a in range(4) for b in range(4) for c in range(2)][1:]
CLASSES = [[o for o in OFFSETS if o[1] == k] for k in (1, 3, 2, 0)]
ORDER = []
while any(CLASSES):
    for group in CLASSES:
        if group:
            ORDER.append(group.pop(0))
PARTS = 4


def lane_gather(tile, index):
    return lax.gather(
        tile,
        index[..., None],
        lax.GatherDimensionNumbers(
            offset_dims=(),
            collapsed_slice_dims=(1,),
            start_index_map=(1,),
            operand_batching_dims=(0,),
            start_indices_batching_dims=(0,),
        ),
        slice_sizes=(1, 1),
        mode=lax.GatherScatterMode.PROMISE_IN_BOUNDS,
    )


def kernel(
    send_hbm, count_hbm, tile_hbm, eps_ref, feat_hbm, near_hbm, degree_hbm, w1_hbm, b1_hbm,
    out_ref, *scratch,
):
    tables, sends, mixes, parcels, owns, rights, fars, lefts = (
        scratch[CHUNKS * k : CHUNKS * (k + 1)] for k in range(8)
    )
    (*index_v, index_0, index_1, index_2, index_3) = scratch[CHUNKS * 8 : CHUNKS * 8 + 2 * RING]
    picks = (index_0, index_1, index_2, index_3)
    (
        send_ref, count_ref, tile_ref, feat_ref, near_ref, degree_ref, w1_ref, b1_ref,
        index_ref, flat_ref, pre_ref, dom_send, dom_recv, feat_send, feat_recv, load_sem,
        ring_send, ring_recv, pick_send, pick_recv, pick_load,
    ) = scratch[CHUNKS * 8 + 2 * RING :]
    loads = [
        pltpu.make_async_copy(src, dst, load_sem.at[i])
        for i, (src, dst) in enumerate(
            (
                (feat_hbm, feat_ref),
                (send_hbm, send_ref),
                (count_hbm, count_ref),
                (tile_hbm, tile_ref),
                (near_hbm, near_ref),
                (degree_hbm, degree_ref),
                (w1_hbm, w1_ref),
                (b1_hbm, b1_ref),
            )
        )
    ]
    for load in loads:
        load.start()
    me = lax.axis_index("dom")
    lane = lax.axis_index("feat")
    x, y, core = me // 8, (me // 2) % RING, me % 2
    first_at, second_at = x + (y - x) * core, y + (x - y) * core
    first_step, second_step = 8 - 6 * core, 2 + 6 * core

    def along(r):
        return me + (lax.rem(first_at + r, RING) - first_at) * first_step

    def across(t, flip):
        return me + (lax.rem(second_at + t, RING) - second_at) * second_step + flip * (1 - 2 * core)

    barrier = pltpu.get_barrier_semaphore()
    for dx, dy, flip in ORDER:
        p = lax.rem(x + dx, RING) * 8 + lax.rem(y + dy, RING) * 2 + lax.rem(core + flip, 2)
        pl.semaphore_signal(barrier, inc=1, device_id={"dom": p}, device_id_type=MESH)
    for step in range(1, FEAT):
        pl.semaphore_signal(barrier, inc=1, device_id={"feat": lax.rem(lane + step, FEAT)}, device_id_type=MESH)

    def ring(c, src, dst, part, k, r):
        pltpu.make_async_remote_copy(
            src_ref=src[c].at[pl.ds(part * HALF, HALF)],
            dst_ref=dst[c].at[pl.ds(part * HALF, HALF)],
            send_sem=ring_send.at[c],
            recv_sem=ring_recv.at[c, k],
            device_id={"dom": along(r)},
            device_id_type=MESH,
        ).start()

    def ring_wait(c, k):
        half = owns[c].at[pl.ds(0, HALF)]
        pltpu.make_async_copy(half, half, ring_recv.at[c, k]).wait()

    def own(c):
        def body(b, carry):
            lanes = pl.ds(pl.multiple_of(b * BLOCK, BLOCK), BLOCK)
            block = feat_ref[c * WIDTH : (c + 1) * WIDTH, lanes]
            owns[c][b] = block
            tables[c][b] = block
            return carry

        lax.fori_loop(0, BLOCKS, body, 0, unroll=4)
        for buffers in (owns, rights, fars, lefts):
            buffers[c][BLOCKS] = jnp.zeros((WIDTH, BLOCK), jnp.bfloat16)

    def wave(c, r):
        source = (owns, rights, fars, lefts)[r][c]
        q = along(r)
        if r > 0:
            for s in range(SLOTS):
                tables[c][BLOCKS + q * SLOTS + s] = source[picks[r][s, me]]
        else:
            for s in range(SLOTS):
                tables[c][BLOCKS + q * SLOTS + s] = jnp.zeros((WIDTH, BLOCK), jnp.bfloat16)
        for k, (t, flip) in enumerate(WAVE):
            p = across(t, flip)
            for s in range(SLOTS):
                sends[c][r * len(WAVE) + k, s] = source[picks[r][s, p]]
        for k, (t, flip) in enumerate(WAVE):
            pltpu.make_async_remote_copy(
                src_ref=sends[c].at[r * len(WAVE) + k],
                dst_ref=tables[c].at[pl.ds(BLOCKS + q * SLOTS, SLOTS)],
                send_sem=dom_send.at[c],
                recv_sem=dom_recv.at[c],
                device_id={"dom": across(t, flip)},
                device_id_type=MESH,
            ).start()

    def forward(c):
        ring_wait(c, 0)
        ring(c, lefts, fars, 0, 4, 1)
        ring_wait(c, 2)
        ring(c, rights, fars, 1, 5, 3)

    def near(c):
        ring_wait(c, 1)
        wave(c, 3)
        ring_wait(c, 3)
        wave(c, 1)

    def far(c):
        ring_wait(c, 4)
        ring_wait(c, 5)
        wave(c, 2)

    for load in loads[:3]:
        load.wait()
    slot = lax.broadcasted_iota(jnp.int32, (SLOTS, DOM), 0)
    index_v[0][...] = jnp.where(slot < count_ref[...], send_ref[...], BLOCKS)
    own_pick = pltpu.make_async_copy(index_v[0], picks[0], pick_load.at[0])
    own_pick.start()
    def hand(r):
        return pltpu.make_async_remote_copy(
            src_ref=index_v[0],
            dst_ref=index_v[r],
            send_sem=pick_send.at[r],
            recv_sem=pick_recv.at[r],
            device_id={"dom": along(RING - r)},
            device_id_type=MESH,
        )

    def direct(c, part):
        if part == 0:
            own(c)
            for s in range(SLOTS):
                tables[c][BLOCKS + me * SLOTS + s] = jnp.zeros((WIDTH, BLOCK), jnp.bfloat16)
        group = list(enumerate(ORDER))[part * len(ORDER) // PARTS : (part + 1) * len(ORDER) // PARTS]

        def peer(offset):
            return (
                lax.rem(x + offset[0], RING) * 8
                + lax.rem(y + offset[1], RING) * 2
                + lax.rem(core + offset[2], 2)
            )

        for k, offset in group:
            p = peer(offset)
            for s in range(SLOTS):
                sends[c][k, s] = owns[c][picks[0][s, p]]
        for k, offset in group:
            pltpu.make_async_remote_copy(
                src_ref=sends[c].at[k],
                dst_ref=tables[c].at[pl.ds(BLOCKS + me * SLOTS, SLOTS)],
                send_sem=dom_send.at[c],
                recv_sem=dom_recv.at[c],
                device_id={"dom": peer(offset)},
                device_id_type=MESH,
            ).start()

    def start(c):
        own(c)
        if c == 0:
            pl.semaphore_wait(barrier, DOM + FEAT - 2)
        ring(c, owns, lefts, 0, 0, 1)
        ring(c, owns, rights, 1, 2, 3)
        ring(c, owns, lefts, 1, 1, 1)
        ring(c, owns, rights, 0, 3, 3)
        if c == 0:
            own_pick.wait()
            for r in range(1, RING):
                hand(r).start()
        wave(c, 0)

    def stage():
        for load in loads[3:]:
            load.wait()

        def body(b, carry):
            lanes = pl.ds(pl.multiple_of(b * BLOCK, BLOCK), BLOCK)
            for j in range(NEIGH):
                flat_ref[b * NEIGH + j] = tile_ref[j, b]
            for j in range(NEIGH):
                index_ref[b, j] = jnp.broadcast_to(near_ref[j : j + 1, lanes], (WIDTH, BLOCK)).astype(jnp.int16)
            return carry

        lax.fori_loop(0, BLOCKS, body, 0)
        for r in range(1, RING):
            hand(r).wait()
        loaded = [pltpu.make_async_copy(index_v[r], picks[r], pick_load.at[r]) for r in range(1, RING)]
        for load in loaded:
            load.start()
        for load in loaded:
            load.wait()

    weight = 1.0 + eps_ref[0]

    def to_feat(c, g):
        return pltpu.make_async_remote_copy(
            src_ref=mixes[c].at[g],
            dst_ref=parcels[c].at[lane],
            send_sem=feat_send.at[c],
            recv_sem=feat_recv.at[c],
            device_id={"feat": g},
            device_id_type=MESH,
        )

    def aggregate(c, first, last):
        table = tables[c]

        def group(i, carry):
            g = lax.rem(lane + 1 + i, FEAT)

            def part(h, inner):
                for u in range(UNROLL):
                    at = h * UNROLL + u
                    b = g * 8 + at
                    limit = jnp.broadcast_to(
                        degree_ref[:, pl.ds(pl.multiple_of(b * BLOCK, BLOCK), BLOCK)], (8, BLOCK)
                    )
                    own = owns[c][b].astype(jnp.float32)
                    low, high = weight * own[:8], weight * own[8:]
                    for j in range(NEIGH):
                        got = lane_gather(table[flat_ref[b * NEIGH + j]], index_ref[b, j]).astype(jnp.float32)
                        live = j < limit
                        low = low + jnp.where(live, got[:8], 0.0)
                        high = high + jnp.where(live, got[8:], 0.0)
                    mixes[c][g, :, pl.ds(pl.multiple_of(at * BLOCK, BLOCK), BLOCK)] = jnp.concatenate(
                        [low, high], 0
                    ).astype(jnp.bfloat16)
                return inner

            lax.fori_loop(0, 8 // UNROLL, part, 0)

            @pl.when(i < FEAT - 1)
            def _():
                to_feat(c, g).start()

            return carry

        if first == 0:
            landed = tables[c].at[pl.ds(BLOCKS, (RING * len(WAVE) if c < RINGS else len(ORDER)) * SLOTS)]
            pltpu.make_async_copy(landed, landed, dom_recv.at[c]).wait()
        lax.fori_loop(first, last, group, 0)
        if last == FEAT:
            parcels[c][lane] = mixes[c][lane]

    def mlp(c, first, last):
        held = parcels[c].at[pl.ds(0, FEAT - 1)]
        pltpu.make_async_copy(held, held, feat_recv.at[c]).wait()
        w1 = jnp.concatenate([w1_ref[f * 64 + c * WIDTH : f * 64 + (c + 1) * WIDTH] for f in range(FEAT)], 0)

        def body(r, carry):
            rows = pl.ds(pl.multiple_of(r * 256, 256), 256)
            cols = parcels[c][:, :, rows].reshape(FEAT * WIDTH, 256)
            part = lax.dot_general(cols, w1, (((0,), (0,)), ((), ())), preferred_element_type=jnp.float32)
            if first:
                pre_ref[rows] = part + b1_ref[...]
            elif not last:
                pre_ref[rows] += part
            else:
                out_ref[rows] = jnp.maximum(pre_ref[rows] + part, 0.0).astype(jnp.bfloat16)
            return carry

        lax.fori_loop(0, OWNED // 256, body, 0)

    merges = [int(step[1]) for step in PLAN if step[0] == "m"]
    for step in PLAN:
        op, c = step[0], ord(step[1]) - 48
        if op == "s":
            start(c)
        elif op == "d":
            direct(RINGS + c // PARTS, c % PARTS)
        elif op == "t":
            stage()
        elif op == "f":
            forward(c)
        elif op == "n":
            near(c)
        elif op == "r":
            far(c)
        elif op == "a":
            aggregate(c, 0, FEAT)
        elif op == "b":
            aggregate(c, 0, FEAT // 2)
        elif op == "e":
            aggregate(c, FEAT // 2, FEAT)
        elif op == "m":
            mlp(c, c == merges[0], c == merges[-1])
    for c in range(CHUNKS):
        pltpu.make_async_copy(sends[c], sends[c], dom_send.at[c]).wait()
        if c < RINGS:
            ringed = tables[c].at[pl.ds(0, 6 * HALF)]
            pltpu.make_async_copy(ringed, ringed, ring_send.at[c]).wait()
        left = mixes[c].at[pl.ds(0, FEAT - 1)]
        pltpu.make_async_copy(left, left, feat_send.at[c]).wait()


def per_device(
    features, send_blocks, counts, tile_blocks, neighbours, degree, epsilon, w_first, b_first, w_second, b_second
):
    smem = pl.BlockSpec(memory_space=pltpu.SMEM)
    vmem = pl.BlockSpec(memory_space=pltpu.VMEM)
    hbm = pl.BlockSpec(memory_space=pl.ANY)
    bf16 = jnp.bfloat16
    int32 = jnp.int32
    hidden = w_first.shape[1]
    activated = pl.pallas_call(
        kernel,
        out_shape=jax.ShapeDtypeStruct((OWNED, hidden), bf16),
        in_specs=[hbm] * 3 + [smem] + [hbm] * 5,
        out_specs=vmem,
        scratch_shapes=[pltpu.VMEM((BLOCKS + DOM * SLOTS, WIDTH, BLOCK), bf16)] * CHUNKS
        + [
            pltpu.VMEM((RING * len(WAVE) if c < RINGS else len(ORDER), SLOTS, WIDTH, BLOCK), bf16)
            for c in range(CHUNKS)
        ]
        + [pltpu.VMEM((FEAT, WIDTH, OWNED), bf16)] * CHUNKS
        + [pltpu.VMEM((FEAT, WIDTH, OWNED), bf16)] * CHUNKS
        + [pltpu.VMEM((BLOCKS + 1, WIDTH, BLOCK), bf16)] * (4 * CHUNKS)
        + [pltpu.VMEM((SLOTS, DOM), int32)] * RING
        + [pltpu.SMEM((SLOTS, DOM), int32)] * RING
        + [
            pltpu.VMEM((SLOTS, DOM), int32),
            pltpu.VMEM((1, DOM), int32),
            pltpu.SMEM((NEIGH, BLOCKS), int32),
            pltpu.VMEM(features.shape, bf16),
            pltpu.VMEM(neighbours.shape, int32),
            pltpu.VMEM((1, degree.shape[0]), int32),
            pltpu.VMEM(w_first.shape, bf16),
            pltpu.VMEM((1, hidden), jnp.float32),
            pltpu.VMEM((BLOCKS, NEIGH, WIDTH, BLOCK), jnp.int16),
            pltpu.SMEM((BLOCKS * NEIGH,), int32),
            pltpu.VMEM((OWNED, hidden), jnp.float32),
        ]
        + [pltpu.SemaphoreType.DMA((CHUNKS,))] * 4
        + [pltpu.SemaphoreType.DMA((8,))]
        + [pltpu.SemaphoreType.DMA((RINGS,)), pltpu.SemaphoreType.DMA((RINGS, 6))]
        + [pltpu.SemaphoreType.DMA((RING,))] * 3,
        compiler_params=pltpu.CompilerParams(
            collective_id=0, has_side_effects=True, vmem_limit_bytes=60 * 1024 * 1024
        ),
        name="gin",
    )(send_blocks[0].T, counts, tile_blocks, epsilon, features, neighbours, degree[None], w_first, b_first[None])
    return (jnp.dot(activated, w_second, preferred_element_type=jnp.float32) + b_second).astype(bf16)


def solution(mesh):
    return jax.shard_map(
        per_device,
        mesh=mesh,
        in_specs=(
            P("feat", "dom"),
            P("dom", None, None),
            P("dom", None),
            P(None, "dom"),
            P(None, "dom"),
            P("dom"),
            P(),
            P(),
            P(),
            P(),
            P(),
        ),
        out_specs=P(("dom", "feat"), None),
        check_vma=False,
    )
```

```python
import functools

import jax
import jax.numpy as jnp
from jax import lax
from jax.experimental import pallas as pl
from jax.experimental.pallas import tpu as pltpu
from jax.sharding import PartitionSpec as P

MESH = pl.DeviceIdType.MESH
BLOCK = 128
DOM = 32
FEAT = 8
SLOTS = 8
NEIGH = 24
BLOCKS = 64
CHUNKS = 4
WIDTH = 16
UNROLL = 8
OWNED = 1024

RING = 4
PLAN = ("s0", "s1", "t0", "f0", "n0", "d0", "f1", "n1", "r0", "d1", "r1", "d2", "d3", "b0", "d4", "d5", "e0", "d6", "d7", "a1", "m0", "a2", "m1", "a3", "m2", "m3")
RINGS = 2
HALF = BLOCKS // 2
WAVE = [(1, 0), (3, 0), (2, 0), (1, 1), (3, 1), (2, 1), (0, 1)]


OFFSETS = [(a, b, c) for a in range(4) for b in range(4) for c in range(2)][1:]
CLASSES = [[o for o in OFFSETS if o[1] == k] for k in (1, 3, 2, 0)]
ORDER = []
while any(CLASSES):
    for group in CLASSES:
        if group:
            ORDER.append(group.pop(0))
PARTS = 4


def lane_gather(tile, index):
    return lax.gather(
        tile,
        index[..., None],
        lax.GatherDimensionNumbers(
            offset_dims=(),
            collapsed_slice_dims=(1,),
            start_index_map=(1,),
            operand_batching_dims=(0,),
            start_indices_batching_dims=(0,),
        ),
        slice_sizes=(1, 1),
        mode=lax.GatherScatterMode.PROMISE_IN_BOUNDS,
    )


def kernel(
    send_hbm, count_hbm, tile_hbm, eps_ref, feat_hbm, near_hbm, degree_hbm, w1_hbm, b1_hbm,
    out_ref, *scratch,
):
    tables, sends, mixes, parcels, owns, rights, fars, lefts = (
        scratch[CHUNKS * k : CHUNKS * (k + 1)] for k in range(8)
    )
    (*index_v, index_0, index_1, index_2, index_3) = scratch[CHUNKS * 8 : CHUNKS * 8 + 2 * RING]
    picks = (index_0, index_1, index_2, index_3)
    (
        send_ref, count_ref, tile_ref, feat_ref, near_ref, degree_ref, w1_ref, b1_ref,
        index_ref, flat_ref, pre_ref, dom_send, dom_recv, feat_send, feat_recv, load_sem,
        ring_send, ring_recv, pick_send, pick_recv, pick_load, act_ref, out_sem,
    ) = scratch[CHUNKS * 8 + 2 * RING :]
    loads = [
        pltpu.make_async_copy(src, dst, load_sem.at[i])
        for i, (src, dst) in enumerate(
            (
                (feat_hbm, feat_ref),
                (send_hbm, send_ref),
                (count_hbm, count_ref),
                (tile_hbm, tile_ref),
                (near_hbm, near_ref),
                (degree_hbm, degree_ref),
                (w1_hbm, w1_ref),
                (b1_hbm, b1_ref),
            )
        )
    ]
    for load in loads:
        load.start()
    me = lax.axis_index("dom")
    lane = lax.axis_index("feat")
    x, y, core = me // 8, (me // 2) % RING, me % 2
    first_at, second_at = x + (y - x) * core, y + (x - y) * core
    first_step, second_step = 8 - 6 * core, 2 + 6 * core

    def along(r):
        return me + (lax.rem(first_at + r, RING) - first_at) * first_step

    def across(t, flip):
        return me + (lax.rem(second_at + t, RING) - second_at) * second_step + flip * (1 - 2 * core)

    barrier = pltpu.get_barrier_semaphore()
    for dx, dy, flip in ORDER:
        p = lax.rem(x + dx, RING) * 8 + lax.rem(y + dy, RING) * 2 + lax.rem(core + flip, 2)
        pl.semaphore_signal(barrier, inc=1, device_id={"dom": p}, device_id_type=MESH)
    for step in range(1, FEAT):
        pl.semaphore_signal(barrier, inc=1, device_id={"feat": lax.rem(lane + step, FEAT)}, device_id_type=MESH)

    def ring(c, src, dst, part, k, r):
        pltpu.make_async_remote_copy(
            src_ref=src[c].at[pl.ds(part * HALF, HALF)],
            dst_ref=dst[c].at[pl.ds(part * HALF, HALF)],
            send_sem=ring_send.at[c],
            recv_sem=ring_recv.at[c, k],
            device_id={"dom": along(r)},
            device_id_type=MESH,
        ).start()

    def ring_wait(c, k):
        half = owns[c].at[pl.ds(0, HALF)]
        pltpu.make_async_copy(half, half, ring_recv.at[c, k]).wait()

    def own(c):
        def body(b, carry):
            lanes = pl.ds(pl.multiple_of(b * BLOCK, BLOCK), BLOCK)
            block = feat_ref[c * WIDTH : (c + 1) * WIDTH, lanes]
            owns[c][b] = block
            tables[c][b] = block
            return carry

        lax.fori_loop(0, BLOCKS, body, 0, unroll=4)
        for buffers in (owns, rights, fars, lefts):
            buffers[c][BLOCKS] = jnp.zeros((WIDTH, BLOCK), jnp.bfloat16)

    def wave(c, r):
        source = (owns, rights, fars, lefts)[r][c]
        q = along(r)
        if r > 0:
            for s in range(SLOTS):
                tables[c][BLOCKS + q * SLOTS + s] = source[picks[r][s, me]]
        else:
            for s in range(SLOTS):
                tables[c][BLOCKS + q * SLOTS + s] = jnp.zeros((WIDTH, BLOCK), jnp.bfloat16)
        for k, (t, flip) in enumerate(WAVE):
            p = across(t, flip)
            for s in range(SLOTS):
                sends[c][r * len(WAVE) + k, s] = source[picks[r][s, p]]
        for k, (t, flip) in enumerate(WAVE):
            pltpu.make_async_remote_copy(
                src_ref=sends[c].at[r * len(WAVE) + k],
                dst_ref=tables[c].at[pl.ds(BLOCKS + q * SLOTS, SLOTS)],
                send_sem=dom_send.at[c],
                recv_sem=dom_recv.at[c],
                device_id={"dom": across(t, flip)},
                device_id_type=MESH,
            ).start()

    def forward(c):
        ring_wait(c, 0)
        ring(c, lefts, fars, 0, 4, 1)
        ring_wait(c, 2)
        ring(c, rights, fars, 1, 5, 3)

    def near(c):
        ring_wait(c, 1)
        wave(c, 3)
        ring_wait(c, 3)
        wave(c, 1)

    def far(c):
        ring_wait(c, 4)
        ring_wait(c, 5)
        wave(c, 2)

    for load in loads[:3]:
        load.wait()
    slot = lax.broadcasted_iota(jnp.int32, (SLOTS, DOM), 0)
    index_v[0][...] = jnp.where(slot < count_ref[...], send_ref[...], BLOCKS)
    own_pick = pltpu.make_async_copy(index_v[0], picks[0], pick_load.at[0])
    own_pick.start()
    def hand(r):
        return pltpu.make_async_remote_copy(
            src_ref=index_v[0],
            dst_ref=index_v[r],
            send_sem=pick_send.at[r],
            recv_sem=pick_recv.at[r],
            device_id={"dom": along(RING - r)},
            device_id_type=MESH,
        )

    def direct(c, part):
        if part == 0:
            own(c)
            for s in range(SLOTS):
                tables[c][BLOCKS + me * SLOTS + s] = jnp.zeros((WIDTH, BLOCK), jnp.bfloat16)
        group = list(enumerate(ORDER))[part * len(ORDER) // PARTS : (part + 1) * len(ORDER) // PARTS]

        def peer(offset):
            return (
                lax.rem(x + offset[0], RING) * 8
                + lax.rem(y + offset[1], RING) * 2
                + lax.rem(core + offset[2], 2)
            )

        for k, offset in group:
            p = peer(offset)
            for s in range(SLOTS):
                sends[c][k, s] = owns[c][picks[0][s, p]]
        for k, offset in group:
            pltpu.make_async_remote_copy(
                src_ref=sends[c].at[k],
                dst_ref=tables[c].at[pl.ds(BLOCKS + me * SLOTS, SLOTS)],
                send_sem=dom_send.at[c],
                recv_sem=dom_recv.at[c],
                device_id={"dom": peer(offset)},
                device_id_type=MESH,
            ).start()

    def start(c):
        own(c)
        if c == 0:
            pl.semaphore_wait(barrier, DOM + FEAT - 2)
        ring(c, owns, lefts, 0, 0, 1)
        ring(c, owns, rights, 1, 2, 3)
        ring(c, owns, lefts, 1, 1, 1)
        ring(c, owns, rights, 0, 3, 3)
        if c == 0:
            own_pick.wait()
            for r in range(1, RING):
                hand(r).start()
        wave(c, 0)

    def stage():
        for load in loads[3:]:
            load.wait()

        def body(b, carry):
            lanes = pl.ds(pl.multiple_of(b * BLOCK, BLOCK), BLOCK)
            for j in range(NEIGH):
                flat_ref[b * NEIGH + j] = tile_ref[j, b]
            for j in range(NEIGH):
                index_ref[b, j] = jnp.broadcast_to(near_ref[j : j + 1, lanes], (WIDTH, BLOCK)).astype(jnp.int16)
            return carry

        lax.fori_loop(0, BLOCKS, body, 0)
        for r in range(1, RING):
            hand(r).wait()
        loaded = [pltpu.make_async_copy(index_v[r], picks[r], pick_load.at[r]) for r in range(1, RING)]
        for load in loaded:
            load.start()
        for load in loaded:
            load.wait()

    weight = 1.0 + eps_ref[0]

    def to_feat(c, g):
        return pltpu.make_async_remote_copy(
            src_ref=mixes[c].at[g],
            dst_ref=parcels[c].at[lane],
            send_sem=feat_send.at[c],
            recv_sem=feat_recv.at[c],
            device_id={"feat": g},
            device_id_type=MESH,
        )

    def aggregate(c, first, last):
        table = tables[c]

        def group(i, carry):
            g = lax.rem(lane + 1 + i, FEAT)

            def part(h, inner):
                for u in range(UNROLL):
                    at = h * UNROLL + u
                    b = g * 8 + at
                    limit = jnp.broadcast_to(
                        degree_ref[:, pl.ds(pl.multiple_of(b * BLOCK, BLOCK), BLOCK)], (8, BLOCK)
                    )
                    own = owns[c][b].astype(jnp.float32)
                    low, high = weight * own[:8], weight * own[8:]
                    for j in range(NEIGH):
                        got = lane_gather(table[flat_ref[b * NEIGH + j]], index_ref[b, j]).astype(jnp.float32)
                        live = j < limit
                        low = low + jnp.where(live, got[:8], 0.0)
                        high = high + jnp.where(live, got[8:], 0.0)
                    mixes[c][g, :, pl.ds(pl.multiple_of(at * BLOCK, BLOCK), BLOCK)] = jnp.concatenate(
                        [low, high], 0
                    ).astype(jnp.bfloat16)
                return inner

            lax.fori_loop(0, 8 // UNROLL, part, 0)

            @pl.when(i < FEAT - 1)
            def _():
                to_feat(c, g).start()

            return carry

        if first == 0:
            landed = tables[c].at[pl.ds(BLOCKS, (RING * len(WAVE) if c < RINGS else len(ORDER)) * SLOTS)]
            pltpu.make_async_copy(landed, landed, dom_recv.at[c]).wait()
        lax.fori_loop(first, last, group, 0)
        if last == FEAT:
            parcels[c][lane] = mixes[c][lane]

    def mlp(c, first, last):
        held = parcels[c].at[pl.ds(0, FEAT - 1)]
        pltpu.make_async_copy(held, held, feat_recv.at[c]).wait()
        w1 = jnp.concatenate([w1_ref[f * 64 + c * WIDTH : f * 64 + (c + 1) * WIDTH] for f in range(FEAT)], 0)

        def body(r, carry):
            rows = pl.ds(pl.multiple_of(r * 256, 256), 256)
            cols = parcels[c][:, :, rows].reshape(FEAT * WIDTH, 256)
            part = lax.dot_general(cols, w1, (((0,), (0,)), ((), ())), preferred_element_type=jnp.float32)
            if first:
                pre_ref[rows] = part + b1_ref[...]
            elif not last:
                pre_ref[rows] += part
            else:
                act_ref[rows] = jnp.maximum(pre_ref[rows] + part, 0.0).astype(jnp.bfloat16)
                pltpu.make_async_copy(act_ref.at[rows], out_ref.at[rows], out_sem).start()
            return carry

        lax.fori_loop(0, OWNED // 256, body, 0)

    merges = [int(step[1]) for step in PLAN if step[0] == "m"]
    for step in PLAN:
        op, c = step[0], ord(step[1]) - 48
        if op == "s":
            start(c)
        elif op == "d":
            direct(RINGS + c // PARTS, c % PARTS)
        elif op == "t":
            stage()
        elif op == "f":
            forward(c)
        elif op == "n":
            near(c)
        elif op == "r":
            far(c)
        elif op == "a":
            aggregate(c, 0, FEAT)
        elif op == "b":
            aggregate(c, 0, FEAT // 2)
        elif op == "e":
            aggregate(c, FEAT // 2, FEAT)
        elif op == "m":
            mlp(c, c == merges[0], c == merges[-1])
    for c in range(CHUNKS):
        pltpu.make_async_copy(sends[c], sends[c], dom_send.at[c]).wait()
        if c < RINGS:
            ringed = tables[c].at[pl.ds(0, 6 * HALF)]
            pltpu.make_async_copy(ringed, ringed, ring_send.at[c]).wait()
        left = mixes[c].at[pl.ds(0, FEAT - 1)]
        pltpu.make_async_copy(left, left, feat_send.at[c]).wait()
    pltpu.make_async_copy(act_ref, out_ref, out_sem).wait()


def per_device(
    features, send_blocks, counts, tile_blocks, neighbours, degree, epsilon, w_first, b_first, w_second, b_second
):
    smem = pl.BlockSpec(memory_space=pltpu.SMEM)
    hbm = pl.BlockSpec(memory_space=pl.ANY)
    bf16 = jnp.bfloat16
    int32 = jnp.int32
    hidden = w_first.shape[1]
    activated = pl.pallas_call(
        kernel,
        out_shape=jax.ShapeDtypeStruct((OWNED, hidden), bf16),
        in_specs=[hbm] * 3 + [smem] + [hbm] * 5,
        out_specs=hbm,
        scratch_shapes=[pltpu.VMEM((BLOCKS + DOM * SLOTS, WIDTH, BLOCK), bf16)] * CHUNKS
        + [
            pltpu.VMEM((RING * len(WAVE) if c < RINGS else len(ORDER), SLOTS, WIDTH, BLOCK), bf16)
            for c in range(CHUNKS)
        ]
        + [pltpu.VMEM((FEAT, WIDTH, OWNED), bf16)] * CHUNKS
        + [pltpu.VMEM((FEAT, WIDTH, OWNED), bf16)] * CHUNKS
        + [pltpu.VMEM((BLOCKS + 1, WIDTH, BLOCK), bf16)] * (4 * CHUNKS)
        + [pltpu.VMEM((SLOTS, DOM), int32)] * RING
        + [pltpu.SMEM((SLOTS, DOM), int32)] * RING
        + [
            pltpu.VMEM((SLOTS, DOM), int32),
            pltpu.VMEM((1, DOM), int32),
            pltpu.SMEM((NEIGH, BLOCKS), int32),
            pltpu.VMEM(features.shape, bf16),
            pltpu.VMEM(neighbours.shape, int32),
            pltpu.VMEM((1, degree.shape[0]), int32),
            pltpu.VMEM(w_first.shape, bf16),
            pltpu.VMEM((1, hidden), jnp.float32),
            pltpu.VMEM((BLOCKS, NEIGH, WIDTH, BLOCK), jnp.int16),
            pltpu.SMEM((BLOCKS * NEIGH,), int32),
            pltpu.VMEM((OWNED, hidden), jnp.float32),
        ]
        + [pltpu.SemaphoreType.DMA((CHUNKS,))] * 4
        + [pltpu.SemaphoreType.DMA((8,))]
        + [pltpu.SemaphoreType.DMA((RINGS,)), pltpu.SemaphoreType.DMA((RINGS, 6))]
        + [pltpu.SemaphoreType.DMA((RING,))] * 3
        + [pltpu.VMEM((OWNED, hidden), bf16), pltpu.SemaphoreType.DMA],
        compiler_params=pltpu.CompilerParams(
            collective_id=0, has_side_effects=True, vmem_limit_bytes=60 * 1024 * 1024
        ),
        name="gin",
    )(send_blocks[0].T, counts, tile_blocks, epsilon, features, neighbours, degree[None], w_first, b_first[None])
    return (jnp.dot(activated, w_second, preferred_element_type=jnp.float32) + b_second).astype(bf16)


def solution(mesh):
    return jax.shard_map(
        per_device,
        mesh=mesh,
        in_specs=(
            P("feat", "dom"),
            P("dom", None, None),
            P("dom", None),
            P(None, "dom"),
            P(None, "dom"),
            P("dom"),
            P(),
            P(),
            P(),
            P(),
            P(),
        ),
        out_specs=P(("dom", "feat"), None),
        check_vma=False,
    )
```
